32 devices in a mesh: dp: 4 (over y, x), fsdp: 8 (over z, core).
Axes of the slice: x: 2, y: 2, z: 4, core: 2. Of those that a mesh axis runs over, the one named last changes fastest.
Arguments:
- grads: bfloat16 [4, 16, 512, 512], P('dp', None, 'fsdp'), may hold values from -4 to 4
- left_stats: float32 [8, 4, 512, 512], P('fsdp', None, 'dp'), may hold values from -0.5 to 9, as said below
- right_stats: float32 [8, 4, 512, 512], P('fsdp', None, 'dp'), may hold values from -0.5 to 9, as said below
- left_root: bfloat16 [8, 4, 512, 512], P('fsdp', None, 'dp'), may hold values from -0.5 to 14, as said below
- right_root: bfloat16 [8, 4, 512, 512], P('fsdp'), may hold values from -0.5 to 14, as said below
- second_moment: float32 [8, 4, 512, 512], P('fsdp', None, 'dp'), may hold values from 0.2 to 2
- slot_block: int32 [8, 4], replicated, may hold values from 0 to 15, as said below
- counts: int32 [8], replicated, may hold values from 0 to 4, as said below
Outputs:
- left_new: float32 [8, 4, 512, 512], P('fsdp', None, 'dp')
- right_new: float32 [8, 4, 512, 512], P('fsdp', None, 'dp')
- second_new: float32 [8, 4, 512, 512], P('fsdp', None, 'dp')
- update: float32 [8, 4, 512, 512], P('fsdp', None, 'dp')
The draws below stay inside these ranges and needn't reach their ends.
Inputs may be any that keep to these rules, and one draw needn't show every extreme that they name: Every owner holds counts[o] blocks; the counts sum to 16, and some owner holds exactly 4. `slot_block`: the first counts[o] slots of owner o name distinct blocks, every block is named by exactly one such slot, and later slots name arbitrary blocks. `left_stats`: Symmetric. `right_stats`: Symmetric. `left_root`: Symmetric. `right_root`: Symmetric.
All inputs are finite; a program needn't handle non-finite values.
Results may differ from the reference program's by a relative error of at most 0.015.
Values may be sent and summed in bfloat16 or wider, within the bound.
No kernel may reach another device: no remote copies, remote signals or barrier semaphores. Data moves between devices by JAX's collectives and lax.ppermute only.
A program may use at most 64 MiB of HBM per device.

```python
import math
import jax
import jax.numpy as jnp
from jax import lax

BS = 512
BLK_OWN = 2
CAP = 4
NB = 16
N_DP = 4
N_FSDP = 8


def symmetric_blocks(key, low_end, high_end):
    noise_key, diag_key = jax.random.split(key, 2)
    block_shape = (N_FSDP, CAP, BS, BS)
    symmetric = jax.random.normal(noise_key, block_shape, jnp.float32)
    diagonal = jnp.exp(jax.random.uniform(diag_key, block_shape[:3], jnp.float32, jnp.log(low_end), jnp.log(high_end)))
    symmetric = (symmetric + jnp.swapaxes(symmetric, 2, 3)) * (0.45 / (2.0 * BS) ** 0.5)
    row_place = jnp.arange(BS, dtype=jnp.float32) / BS
    diagonal = diagonal * 3.0 ** row_place
    return symmetric + diagonal[..., None] * jnp.eye(BS, dtype=jnp.float32)


def ownership(key):
    base_key = jax.random.fold_in(key, 77)
    owner_key, shift_key, block_key = jax.random.split(base_key, 3)
    owners = jax.random.permutation(owner_key, N_FSDP)
    half_owners = N_FSDP // 2
    moved_blocks = jax.random.randint(shift_key, (half_owners,), 0, BLK_OWN + 1)
    moved_blocks = moved_blocks.at[0].set(BLK_OWN)
    held = jnp.full((N_FSDP,), BLK_OWN, jnp.int32)
    held = held.at[owners[:half_owners]].add(moved_blocks).at[owners[half_owners:]].add(-moved_blocks)
    blocks = jax.random.permutation(block_key, NB)
    offsets = jnp.cumsum(held) - held
    slot_place = (offsets[:, None] + jnp.arange(CAP)[None, :]) % NB
    return (held.astype(jnp.int32), blocks[slot_place].astype(jnp.int32))


def draw_left_stats(key, part):
    return symmetric_blocks(jax.random.fold_in(key, 1), 0.5, 2.0)


def draw_right_stats(key, part):
    return symmetric_blocks(jax.random.fold_in(key, 2), 0.5, 2.0)


def draw_left_root(key, part):
    return symmetric_blocks(jax.random.fold_in(key, 3), 1.0, 3.3).astype(jnp.bfloat16)


def draw_right_root(key, part):
    return symmetric_blocks(jax.random.fold_in(key, 4), 1.0, 3.3).astype(jnp.bfloat16)


def draw_slot_block(key, part):
    return ownership(key)[1]


def draw_counts(key, part):
    return ownership(key)[0]


def block_scale(key, shape, shards, least, top_value):
    gain, own = 1.0, jax.random.fold_in(key, 6)
    for axis_at, blocks in shards:
        heights = jnp.exp(jax.random.uniform(jax.random.fold_in(own, axis_at), (blocks,), jnp.float32, least / len(shards), top_value / len(shards)))
        gain = gain * jnp.repeat(heights, shape[axis_at] // blocks).reshape([-1 if axis == axis_at else 1 for axis in range(len(shape))])
    return gain


def centred(rng, extent, scale, reach, pieces=(), kind=jnp.bfloat16):
    result = scale * jax.random.normal(rng, extent, jnp.float32)
    if pieces:
        result = result * block_scale(rng, extent, pieces, -0.22, 0.18)
    return jnp.clip(result, -reach, reach).astype(kind)


def setup_inputs(seed: int = 0) -> dict:
    arg_keys = jax.random.split(jax.random.key(seed), 9)
    grads = centred(arg_keys[0], (N_DP, NB, BS, BS), 0.25, 4.0, ((0, 4), (2, 8)))
    left_stats = draw_left_stats(jax.random.fold_in(arg_keys[8], 71), 0)
    right_stats = draw_right_stats(jax.random.fold_in(arg_keys[8], 71), 0)
    left_root = draw_left_root(jax.random.fold_in(arg_keys[8], 71), 0)
    right_root = draw_right_root(jax.random.fold_in(arg_keys[8], 71), 0)
    second_moment = jnp.clip(jnp.exp(math.log(2.0) - 2.3025851 * jax.random.uniform(arg_keys[5], (N_FSDP, CAP, BS, BS), jnp.float32) ** block_scale(arg_keys[5], (N_FSDP, CAP, BS, BS), ((0, 8), (2, 4)), -0.2, 0.2)), 0.2, 2.0)
    slot_block = draw_slot_block(jax.random.fold_in(arg_keys[8], 71), 0)
    counts = draw_counts(jax.random.fold_in(arg_keys[8], 71), 0)
    return {"grads": grads, "left_stats": left_stats, "right_stats": right_stats, "left_root": left_root, "right_root": right_root, "second_moment": second_moment, "slot_block": slot_block, "counts": counts}


SHAMPOO_BETA = 0.998
ADAM_BETA = 0.95
EPSILON = 1e-08

def reference(grads, left_stats, right_stats, left_root, right_root, second_moment, slot_block, counts):

    def accumulate(step_index, grad_total):
        return grad_total + grads[step_index].astype(jnp.float32)
    grad_total = lax.fori_loop(0, N_DP, accumulate, jnp.zeros(grads.shape[1:], jnp.float32))
    grad_blocks = lax.optimization_barrier(grad_total.astype(jnp.bfloat16))
    live_slots = jnp.arange(CAP, dtype=jnp.int32)[None, :] < counts[:, None]
    keep_mask = live_slots[:, :, None, None]
    picked = jnp.where(keep_mask, grad_blocks[slot_block], jnp.zeros((), jnp.bfloat16))
    widened = picked.astype(jnp.float32)
    left_term = jnp.einsum('oaik,oajk->oaij', widened, widened)
    right_term = jnp.einsum('oaki,oakj->oaij', widened, widened)
    left_new = jnp.where(keep_mask, SHAMPOO_BETA * left_stats + (1.0 - SHAMPOO_BETA) * left_term, left_stats)
    right_new = jnp.where(keep_mask, SHAMPOO_BETA * right_stats + (1.0 - SHAMPOO_BETA) * right_term, right_stats)
    left_half = jnp.einsum('oaik,oakj->oaij', left_root.astype(jnp.float32), widened)
    left_half = lax.optimization_barrier(left_half.astype(jnp.bfloat16))
    precond = jnp.einsum('oaik,oakj->oaij', left_half.astype(jnp.float32), right_root.astype(jnp.float32))
    second_new = jnp.where(keep_mask, ADAM_BETA * second_moment + (1.0 - ADAM_BETA) * widened * widened, second_moment)
    adam = widened / (jnp.sqrt(second_new) + EPSILON)
    precond_sum = lax.optimization_barrier(jnp.sum(precond * precond, axis=(2, 3)))
    adam_sum = lax.optimization_barrier(jnp.sum(adam * adam, axis=(2, 3)))
    graft_scale = jnp.where(live_slots, jnp.sqrt(adam_sum / jnp.where(live_slots, precond_sum, 1.0)), 0.0)
    update = precond * graft_scale[:, :, None, None]
    return (left_new, right_new, second_new, update)
```

```python
import functools

import jax
import jax.numpy as jnp
from jax import lax
from jax.experimental import pallas as pl
from jax.experimental.pallas import tpu as pltpu
from jax.sharding import PartitionSpec as P

SHAMPOO_BETA = 0.998
ADAM_BETA = 0.95
EPSILON = 1e-08
VMEM_LIMIT = 48 * 1024 * 1024
SMEM = pltpu.SMEM
VMEM = pltpu.VMEM


def owner_start(counts_ref, owner):
    def add(at, total):
        return total + jnp.where(at < owner, counts_ref[at], 0)

    return lax.fori_loop(0, counts_ref.shape[0], add, jnp.int32(0), unroll=True)


def exchange(value, axis, distance):
    size = lax.axis_size(axis)
    return lax.ppermute(value, axis, [(i, i ^ distance) for i in range(size)])


def deal_kernel(slot_block, counts, grads, *rest):
    outs, (order, sems) = rest[:-2], rest[-2:]
    ways = len(outs)
    owners, cap = slot_block.shape
    place = jnp.int32(0)
    for owner in range(owners):
        for slot in range(cap):
            @pl.when(slot < counts[owner])
            def _():
                order[place + slot] = slot_block[owner, slot]
        place = place + counts[owner]
    me = lax.axis_index("dp")
    copies = []
    for distance in list(range(1, ways)) + [0]:
        for at in range(outs[0].shape[0]):
            block = order[at * ways + (me ^ distance)]
            copies.append(
                pltpu.make_async_copy(
                    grads.at[block], outs[distance].at[at], sems.at[distance * outs[0].shape[0] + at]
                )
            )
            copies[-1].start()
    for copy in copies:
        copy.wait()


def deal(slot_block, counts, grads, ways):
    blocks, rows, width = grads.shape
    group = jax.ShapeDtypeStruct((blocks // ways, rows, width), grads.dtype)
    return pl.pallas_call(
        deal_kernel,
        out_shape=(group,) * ways,
        in_specs=[
            pl.BlockSpec(memory_space=SMEM),
            pl.BlockSpec(memory_space=SMEM),
            pl.BlockSpec(memory_space=pl.ANY),
        ],
        out_specs=(pl.BlockSpec(memory_space=VMEM),) * ways,
        scratch_shapes=[SMEM((blocks,), jnp.int32), pltpu.SemaphoreType.DMA((blocks,))],
        name="deal",
    )(slot_block, counts, grads)


def route_kernel(counts, *rest):
    parts, (out, held) = rest[:-2], rest[-2:]
    ways = len(parts)
    total = parts[0][...].astype(jnp.float32)
    for part in parts[1:]:
        total = total + part[...].astype(jnp.float32)
    held[...] = total.astype(held.dtype)
    me = lax.axis_index("dp")
    start = jnp.int32(0)
    for owner in range(out.shape[0]):
        slot = (me - start + 2 * out.shape[0] * ways) % ways
        at = jnp.where(slot < counts[owner], (start + slot) // ways, 0)
        out[owner] = held[at]
        start = start + counts[owner]


def route(counts, parts, owners):
    group = parts[0].shape
    return pl.pallas_call(
        route_kernel,
        out_shape=jax.ShapeDtypeStruct((owners,) + group[1:], parts[0].dtype),
        in_specs=[pl.BlockSpec(memory_space=SMEM)] + [pl.BlockSpec(memory_space=VMEM)] * len(parts),
        out_specs=pl.BlockSpec(memory_space=VMEM),
        scratch_shapes=[VMEM(group, parts[0].dtype)],
        name="route",
    )(counts, *parts)


def direct_kernel(meta, grad, root, right, moment, *rest):
    precond_out, moment_out, norms = rest[-3:]
    step = pl.program_id(0)
    live = meta[step] < meta[meta.shape[0] - 1]
    rows = root.shape[1]
    place = pl.multiple_of(lax.axis_index("dp") * rows, rows)
    half = jnp.dot(root[0], grad[0], preferred_element_type=jnp.float32).astype(jnp.bfloat16)
    precond = jnp.dot(half, right[0], preferred_element_type=jnp.float32)
    precond_out[0] = precond
    values = grad[0, pl.ds(place, rows), :].astype(jnp.float32)
    old = moment[0]
    new = jnp.where(live, ADAM_BETA * old + (1.0 - ADAM_BETA) * values * values, old)
    moment_out[0] = new
    adam = values / (jnp.sqrt(new) + EPSILON)
    norms[0, 0:1, :] = jnp.full((1, 128), jnp.sum(precond * precond), jnp.float32)
    norms[0, 1:2, :] = jnp.full((1, 128), jnp.sum(adam * adam), jnp.float32)


def direct(meta, grad, root, right, moment, carried):
    count = grad.shape[0]
    slots, rows, width = moment.shape
    by_slot = lambda i, m: (m[i], 0, 0)
    state = pl.BlockSpec((1, rows, width), by_slot)
    kept = [] if carried is None else list(carried)
    big = jax.ShapeDtypeStruct((slots, rows, width), jnp.float32)
    return pl.pallas_call(
        direct_kernel,
        out_shape=(big, big, jax.ShapeDtypeStruct((slots, 8, 128), jnp.float32)),
        grid_spec=pltpu.PrefetchScalarGridSpec(
            num_scalar_prefetch=1,
            grid=(count,),
            in_specs=[
                pl.BlockSpec((1, width, width), lambda i, m: (i, 0, 0)),
                state,
                pl.BlockSpec((1, width, width), by_slot),
                state,
            ]
            + [pl.BlockSpec(memory_space=pl.ANY)] * len(kept),
            out_specs=(state, state, pl.BlockSpec((1, 8, 128), by_slot)),
        ),
        input_output_aliases={5 + i: i for i in range(len(kept))},
        compiler_params=pltpu.CompilerParams(vmem_limit_bytes=VMEM_LIMIT),
        cost_estimate=pl.CostEstimate(
            flops=count * 4 * rows * width * width * 4, bytes_accessed=count * 2_000_000, transcendentals=0
        ),
        name="direct",
    )(meta, grad, root, right, moment, *kept)


def gram_kernel(meta, grad, left, right, *rest):
    left_out, right_out = rest[-2:]
    step = pl.program_id(0)
    live = meta[step] < meta[meta.shape[0] - 1]
    rows = left.shape[1]
    place = pl.multiple_of(lax.axis_index("dp") * rows, rows)
    whole = grad[0]
    across = lax.dot_general(
        grad[0, pl.ds(place, rows), :], whole, (((1,), (1,)), ((), ())), preferred_element_type=jnp.float32
    )
    down = lax.dot_general(
        grad[0, :, pl.ds(place, rows)], whole, (((0,), (0,)), ((), ())), preferred_element_type=jnp.float32
    )
    left_old = left[0]
    right_old = right[0]
    left_out[0] = jnp.where(live, SHAMPOO_BETA * left_old + (1.0 - SHAMPOO_BETA) * across, left_old)
    right_out[0] = jnp.where(live, SHAMPOO_BETA * right_old + (1.0 - SHAMPOO_BETA) * down, right_old)


def gram(meta, grad, left, right, carried):
    count = grad.shape[0]
    slots, rows, width = left.shape
    by_slot = lambda i, m: (m[i], 0, 0)
    state = pl.BlockSpec((1, rows, width), by_slot)
    kept = [] if carried is None else list(carried)
    big = jax.ShapeDtypeStruct((slots, rows, width), jnp.float32)
    return pl.pallas_call(
        gram_kernel,
        out_shape=(big, big),
        grid_spec=pltpu.PrefetchScalarGridSpec(
            num_scalar_prefetch=1,
            grid=(count,),
            in_specs=[pl.BlockSpec((1, width, width), lambda i, m: (i, 0, 0)), state, state]
            + [pl.BlockSpec(memory_space=pl.ANY)] * len(kept),
            out_specs=(state, state),
        ),
        input_output_aliases={4 + i: i for i in range(len(kept))},
        compiler_params=pltpu.CompilerParams(vmem_limit_bytes=VMEM_LIMIT),
        cost_estimate=pl.CostEstimate(
            flops=count * 4 * rows * width * width * 4, bytes_accessed=count * 2_000_000, transcendentals=0
        ),
        name="gram",
    )(meta, grad, left, right, *kept)


def graft_kernel(meta, precond, *rest):
    norms, out = rest[:-1], rest[-1]
    slot = pl.program_id(0)
    live = slot < meta[meta.shape[0] - 1]
    total = norms[0][0]
    for part in norms[1:]:
        total = total + part[0]
    precond_sum = jnp.where(live, total[0:1, :], 1.0)
    scale = jnp.where(live, jnp.sqrt(total[1:2, :] / precond_sum), 0.0)
    width = out.shape[2]
    for at in range(0, width, 128):
        value = precond[0, :, at : at + 128]
        out[0, :, at : at + 128] = jnp.where(live, value * scale, 0.0)


def graft(meta, precond, norms):
    slots, rows, width = precond.shape
    state = pl.BlockSpec((1, rows, width), lambda i, m: (i, 0, 0))
    small = pl.BlockSpec((1, 8, 128), lambda i, m: (i, 0, 0))
    return pl.pallas_call(
        graft_kernel,
        out_shape=jax.ShapeDtypeStruct(precond.shape, jnp.float32),
        grid_spec=pltpu.PrefetchScalarGridSpec(
            num_scalar_prefetch=1, grid=(slots,), in_specs=[state] + [small] * len(norms), out_specs=state
        ),
        name="graft",
    )(meta, precond, *norms)


def on_device_direct(
    grads, left_stats, right_stats, left_root, right_root, second_moment, slot_block, counts
):
    ways = lax.axis_size("dp")
    owners = slot_block.shape[0]
    width = left_root.shape[3]
    own, *away = deal(slot_block, counts, grads[0], ways)
    parts = [own] + [exchange(away[k - 1], "dp", k) for k in range(1, ways)]
    routed = route(counts, parts, owners)
    block = lax.all_to_all(routed, "fsdp", split_axis=0, concat_axis=0, tiled=True)
    block = block.reshape(1, width, width)

    me, owner = lax.axis_index("dp"), lax.axis_index("fsdp")
    start = jnp.sum(jnp.where(jnp.arange(owners) < owner, counts, 0))
    held = jnp.sum(jnp.where(jnp.arange(owners) == owner, counts, 0))

    def meta_of(*distances):
        return jnp.stack([((me ^ k) - start + owners * ways * 2) % ways for k in distances] + [held]).astype(jnp.int32)

    side = exchange(block, "dp", 1)
    over = exchange(block, "dp", 2)
    across = jnp.concatenate(
        [exchange(side[:, : width // 2], "dp", 2), exchange(over[:, width // 2 :], "dp", 1)], axis=1
    )
    first = (left_root[0], right_root[0], second_moment[0])
    second = (left_stats[0], right_stats[0])
    acc = direct(meta_of(0), block, *first, None)
    acc = direct(meta_of(1), side, *first, acc)
    acc = direct(meta_of(2), over, *first, acc)
    stats = gram(meta_of(0), block, *second, None)
    stats = gram(meta_of(1), side, *second, stats)
    precond, second_new, norms = direct(meta_of(3), across, *first, acc)
    all_norms = [norms] + [exchange(norms, "dp", k) for k in range(1, ways)]
    stats = gram(meta_of(2), over, *second, stats)
    left_new, right_new = gram(meta_of(3), across, *second, stats)
    update = graft(meta_of(0), precond, all_norms)
    return (left_new[None], right_new[None], second_new[None], update[None])


def on_device(
    grads, left_stats, right_stats, left_root, right_root, second_moment, slot_block, counts
):
    slot_count = slot_block.shape[1]
    owner_count = slot_block.shape[0]
    block_order = left_root.shape[3]
    partial_value = grads[0]
    block_count = partial_value.shape[0]
    slab_rows = partial_value.shape[1]
    flat_slots = slot_block.reshape(-1)
    live_slots = (jnp.arange(slot_count, dtype=jnp.int32)[None, :] < counts[:, None]).reshape(-1)
    flat_partial = partial_value.reshape(block_count, slab_rows * block_order).astype(jnp.float32)
    summed = lax.psum_scatter(
        flat_partial.astype(jnp.bfloat16), "dp", scatter_dimension=1, tiled=True
    )
    picked = jnp.where(live_slots[:, None], summed[flat_slots], jnp.zeros((), jnp.bfloat16))
    received = lax.all_to_all(picked, "fsdp", split_axis=0, concat_axis=1, tiled=True)
    piece_width = summed.shape[1]
    received = received.reshape(slot_count, owner_count, piece_width)
    gathered = lax.all_gather(received, "dp", axis=2, tiled=True)
    grad_full = gathered.reshape(slot_count, block_order, block_order)
    slab_width = block_order // lax.axis_size("dp")
    row_start = lax.axis_index("dp") * slab_width
    row_grad = lax.dynamic_slice_in_dim(grad_full, row_start, slab_width, 1)
    column_grad = lax.dynamic_slice_in_dim(grad_full, row_start, slab_width, 2)
    owned_here = jnp.arange(slot_count, dtype=jnp.int32) < counts[lax.axis_index("fsdp")]
    keep_mask = owned_here[:, None, None]
    left_term = jnp.einsum("crk,cjk->crj", row_grad, grad_full, preferred_element_type=jnp.float32)
    right_term = jnp.einsum(
        "ckr,ckj->crj", column_grad, grad_full, preferred_element_type=jnp.float32
    )
    left_old = left_stats[0]
    right_old = right_stats[0]
    left_new = jnp.where(
        keep_mask, SHAMPOO_BETA * left_old + (1.0 - SHAMPOO_BETA) * left_term, left_old
    )
    right_new = jnp.where(
        keep_mask, SHAMPOO_BETA * right_old + (1.0 - SHAMPOO_BETA) * right_term, right_old
    )
    left_half = jnp.einsum(
        "crk,ckj->crj", left_root[0], grad_full, preferred_element_type=jnp.float32
    ).astype(jnp.bfloat16)
    precond = jnp.einsum(
        "crk,ckj->crj", left_half, right_root[0], preferred_element_type=jnp.float32
    )
    row_values = row_grad.astype(jnp.float32)
    moment_old = second_moment[0]
    second_new = jnp.where(
        keep_mask, ADAM_BETA * moment_old + (1.0 - ADAM_BETA) * row_values * row_values, moment_old
    )
    adam = row_values / (jnp.sqrt(second_new) + EPSILON)
    precond_sum, adam_sum = lax.psum(
        (jnp.sum(precond * precond, axis=(1, 2)), jnp.sum(adam * adam, axis=(1, 2))), "dp"
    )
    graft_scale = jnp.where(
        owned_here, jnp.sqrt(adam_sum / jnp.where(owned_here, precond_sum, 1.0)), 0.0
    )
    update = precond * graft_scale[:, None, None]
    return (left_new[None], right_new[None], second_new[None], update[None])


def solution(mesh):
    in_specs = (
        P("dp", None, "fsdp", None),
        P("fsdp", None, "dp", None),
        P("fsdp", None, "dp", None),
        P("fsdp", None, "dp", None),
        P("fsdp", None, None, None),
        P("fsdp", None, "dp", None),
        P(),
        P(),
    )
    out_specs = (
        P("fsdp", None, "dp", None),
        P("fsdp", None, "dp", None),
        P("fsdp", None, "dp", None),
        P("fsdp", None, "dp", None),
    )

    def body(*args):
        ways, slots = mesh.shape["dp"], args[6].shape[1]
        four = ways == 4 and slots == ways and args[0].shape[1] % ways == 0
        return (on_device_direct if four else on_device)(*args)

    return jax.shard_map(body, mesh=mesh, in_specs=in_specs, out_specs=out_specs, check_vma=False)
```

```python
import functools

import jax
import jax.numpy as jnp
from jax import lax
from jax.experimental import pallas as pl
from jax.experimental.pallas import tpu as pltpu
from jax.sharding import PartitionSpec as P


SHAMPOO_BETA = 0.998
ADAM_BETA = 0.95
EPSILON = 1e-08
SMALL = 8 * 1024 * 1024
SMEM = pltpu.SMEM
VMEM = pltpu.VMEM


def exchange(value, axis, distance):
    size = lax.axis_size(axis)
    return lax.ppermute(value, axis, [(i, i ^ distance) for i in range(size)])


def in_hbm(value):
    return pltpu.with_memory_space_constraint(value, pltpu.HBM)


def in_vmem(value):
    return pltpu.with_memory_space_constraint(value, pltpu.VMEM)


def call(kernel, out, ins, in_specs, out_specs, scratch=(), **more):
    return pl.pallas_call(
        kernel,
        out_shape=out,
        in_specs=in_specs,
        out_specs=out_specs,
        scratch_shapes=list(scratch),
        compiler_params=pltpu.CompilerParams(vmem_limit_bytes=SMALL),
        cost_estimate=pl.CostEstimate(flops=10_000_000, bytes_accessed=1_000_000, transcendentals=0),
        **more,
    )(*ins)


IN_SMEM = pl.BlockSpec(memory_space=SMEM)
IN_VMEM = pl.BlockSpec(memory_space=VMEM)
IN_HBM = pl.BlockSpec(memory_space=pltpu.HBM)


def slot_index(counts, meta, ways):
    me, owner_here, owners = lax.axis_index("dp"), lax.axis_index("fsdp"), counts.shape[0]
    start = jnp.int32(0)
    for owner in range(owners):
        start = start + jnp.where(owner < owner_here, counts[owner], 0)
    for distance in range(ways):
        meta[distance] = ((me ^ distance) - start + owners * ways * 2) % ways
    meta[ways] = counts[owner_here]


def deal_kernel(part, chunks, slot_block, counts, grads, *rest):
    outs, (order, sems) = rest[:-2], rest[-2:]
    ways, group = len(outs), outs[0].shape[0]
    cap, owners = slot_block.shape
    me = lax.axis_index("dp")
    place = jnp.int32(0)
    for owner in range(owners):
        for slot in range(cap):

            @pl.when(slot < counts[owner])
            def _():
                order[place + slot] = slot_block[slot, owner]

        place = place + counts[owner]
    rows = grads.shape[1] // chunks
    copies = []
    for distance in list(range(1, ways)) + [0]:
        for at in range(group):
            block = order[at * ways + (me ^ distance)]
            sem = sems.at[distance * group + at]
            copy = pltpu.make_async_copy(grads.at[block, pl.ds(part * rows, rows)], outs[distance].at[at], sem)
            copy.start()
            copies.append(copy)
    for copy in copies:
        copy.wait()


def deal(slot_block, counts, grads, ways, part, chunks):
    blocks, rows, width = grads.shape
    return call(
        functools.partial(deal_kernel, part, chunks),
        (pltpu.VMEM((blocks // ways, rows // chunks, width), grads.dtype),) * ways,
        (in_hbm(slot_block.T), in_hbm(counts), in_hbm(grads)),
        [IN_SMEM, IN_SMEM, IN_HBM],
        (IN_VMEM,) * ways,
        [SMEM((blocks,), jnp.int32), pltpu.SemaphoreType.DMA((blocks,))],
    )


def ready_kernel(ways, counts, root, moment, meta, lent, wide, sems):
    slot_index(counts, meta, ways)
    slot = meta[ways - 1]
    near = pltpu.make_async_copy(root.at[slot], lent.at[0], sems.at[0])
    far = pltpu.make_async_copy(moment.at[slot], wide, sems.at[1])
    near.start()
    far.start()
    far.wait()
    lent[1] = wide[...].astype(lent.dtype)
    near.wait()


def ready(counts, root, moment, ways):
    _, high, wide = root.shape
    return call(
        functools.partial(ready_kernel, ways),
        (jax.ShapeDtypeStruct((ways + 1,), jnp.int32), pltpu.VMEM((2, high, wide), jnp.bfloat16)),
        (in_hbm(counts), in_hbm(root), in_hbm(moment)),
        [IN_SMEM, IN_HBM, IN_HBM],
        (IN_SMEM, IN_VMEM),
        [VMEM((high, wide), jnp.float32), pltpu.SemaphoreType.DMA((2,))],
    )


def fetch_kernel(*refs):
    count = len(refs) // 2
    sources, outs, sems = refs[:count], refs[count:-1], refs[-1]
    copies = [pltpu.make_async_copy(a, b, sems.at[at]) for at, (a, b) in enumerate(zip(sources, outs))]
    for copy in copies:
        copy.start()
    for copy in copies:
        copy.wait()


def fetch(arrays):
    return call(
        fetch_kernel,
        tuple(pltpu.VMEM(x.shape, x.dtype) for x in arrays),
        [in_hbm(x) for x in arrays],
        [IN_HBM] * len(arrays),
        (IN_VMEM,) * len(arrays),
        [pltpu.SemaphoreType.DMA((len(arrays),))],
    )


def add_parts(parts, held):
    total = parts[0][...].astype(jnp.float32)
    for part in parts[1:]:
        total = total + part[...].astype(jnp.float32)
    held[...] = total.astype(held.dtype)


def piece_of(counts, owner, ways):
    start = jnp.int32(0)
    for at in range(counts.shape[0]):
        start = start + jnp.where(at < owner, counts[at], 0)
    slot = (lax.axis_index("dp") - start + counts.shape[0] * ways * 2) % ways
    return jnp.where(slot < counts[owner], (start + slot) // ways, 0)


def sort_kernel(counts, *rest):
    parts, (same, other, held) = rest[:-3], rest[-3:]
    add_parts(parts, held)
    owner_here = lax.axis_index("fsdp")
    for distance in range(same.shape[0]):
        same[distance] = held[piece_of(counts, owner_here ^ (2 * distance), len(parts))]
        other[distance] = held[piece_of(counts, owner_here ^ (2 * distance + 1), len(parts))]


def sort(counts, parts, owners):
    group = parts[0].shape
    half = pltpu.VMEM((owners // 2,) + group[1:], parts[0].dtype)
    return call(
        sort_kernel,
        (half, half),
        (in_hbm(counts), *[in_vmem(x) for x in parts]),
        [IN_SMEM] + [IN_VMEM] * len(parts),
        (IN_VMEM, IN_VMEM),
        [VMEM(group, parts[0].dtype)],
    )


def pair_kernel(same, other, *outs):
    for at, out in enumerate(outs):
        out[0] = same[at + 1]
        out[1] = other[at + 1]


def pair(same, other):
    out = pltpu.VMEM((2,) + same.shape[1:], same.dtype)
    count = same.shape[0] - 1
    return call(pair_kernel, (out,) * count, (in_vmem(same), in_vmem(other)), [IN_VMEM] * 2, (IN_VMEM,) * count)


def land_kernel(same, other, *rest):
    got, out = rest[:-1], rest[-1]
    me = lax.axis_index("fsdp")
    out[me] = same[0]
    out[me ^ 1] = other[0]
    for at, pieces in enumerate(got):
        out[me ^ (2 * at + 2)] = pieces[0]
        out[me ^ (2 * at + 3)] = pieces[1]


def land(same, other, got):
    out = pltpu.VMEM((2 * same.shape[0],) + same.shape[1:], same.dtype)
    ins = [in_vmem(x) for x in (same, other, *got)]
    return call(land_kernel, out, ins, [IN_VMEM] * len(ins), IN_VMEM)


def assemble(whole, pieces):
    slabs, rows, _ = pieces[0].shape
    for slab in range(slabs):
        for part, piece in enumerate(pieces):
            at = (slab * len(pieces) + part) * rows
            whole[at : at + rows, :] = piece[slab]


def precondition(root, whole, right):
    half = jnp.dot(root, whole[...], preferred_element_type=jnp.float32).astype(jnp.bfloat16)
    return jnp.dot(half, right, preferred_element_type=jnp.float32)


def own_rows(device, rows):
    return pl.ds(pl.multiple_of(device * rows, rows), rows)


def second_of(live, old, values):
    return jnp.where(live, ADAM_BETA * old + (1.0 - ADAM_BETA) * values * values, old)


def norms_of(precond, values, moment):
    adam = values / (jnp.sqrt(moment) + EPSILON)
    return jnp.sum(precond * precond), jnp.sum(adam * adam)


def put_norms(kept, slot, sums):
    row = lax.broadcasted_iota(jnp.int32, kept.shape, 0)
    return jnp.where(row == 2 * slot, sums[0], jnp.where(row == 2 * slot + 1, sums[1], kept))


class Writes:
    def __init__(self, stage, sems):
        self.stage, self.sems, self.copies = stage, sems, []

    def put(self, value, out, slot):
        at = len(self.copies)
        self.stage[at] = value
        self.copies.append(pltpu.make_async_copy(self.stage.at[at], out.at[slot], self.sems.at[at]))
        self.copies[-1].start()

    def wait(self):
        for copy in self.copies:
            copy.wait()


def work_direct(slot, live, whole, root, right, moment, precond_out, moment_out, writes):
    precond = precondition(root[slot], whole, right[slot])
    if precond_out is not None:
        precond_out[slot] = precond
    values = whole[own_rows(lax.axis_index("dp"), root.shape[1]), :].astype(jnp.float32)
    new = second_of(live, moment[slot], values)
    writes.put(new, moment_out, slot)
    return precond, values, new


def work_gram(slot, live, whole, left, right, left_out, right_out, writes):
    rows = own_rows(lax.axis_index("dp"), left.shape[1])
    for part, dims, old, out in (
        (whole[rows, :], ((1,), (1,)), left, left_out),
        (whole[:, rows], ((0,), (0,)), right, right_out),
    ):
        term = lax.dot_general(part, whole[...], (dims, ((), ())), preferred_element_type=jnp.float32)
        kept = old[slot]
        writes.put(jnp.where(live, SHAMPOO_BETA * kept + (1.0 - SHAMPOO_BETA) * term, kept), out, slot)


def own_kernel(ways, meta, a, b, root, right, moment, left, right_stats, lent, *rest):
    precond_out, moment_out, norms, left_out, right_out, whole, stage, sems = rest
    writes = Writes(stage, sems)
    assemble(whole, (a, b))
    slot, held = meta[0], meta[ways]
    live = slot < held
    sums = norms_of(*work_direct(slot, live, whole, root, right, moment, precond_out, moment_out, writes))
    values = whole[own_rows(lax.axis_index("dp") ^ (ways - 1), root.shape[1]), :].astype(jnp.float32)
    there = precondition(lent[0], whole, right[slot])
    more = norms_of(there, values, second_of(live, lent[1].astype(jnp.float32), values))
    norms[...] = put_norms(jnp.zeros(norms.shape, jnp.float32), slot, (sums[0] + more[0], sums[1] + more[1]))
    work_gram(slot, live, whole, left, right_stats, left_out, right_out, writes)
    writes.wait()


def beside_kernel(ways, meta, a0, b0, a1, b1, root, right, moment, kept0, kept1, norms_in, *rest):
    precond_out, moment_out, norms, whole, stage, sems = rest
    writes = Writes(stage, sems)
    total = norms_in[...]
    for distance, pieces in ((1, (a0, b0)), (2, (a1, b1))):
        assemble(whole.at[distance - 1], pieces)
        slot = meta[distance]
        live = slot < meta[ways]
        got = work_direct(slot, live, whole.at[distance - 1], root, right, moment, precond_out, moment_out, writes)
        total = put_norms(total, slot, norms_of(*got))
    norms[...] = total
    writes.wait()


def gram_kernel(ways, meta, a0, b0, a1, b1, left, right_stats, kept0, kept1, *rest):
    left_out, right_out, whole, stage, sems = rest
    writes = Writes(stage, sems)
    for distance, pieces in ((1, (a0, b0)), (2, (a1, b1))):
        assemble(whole.at[distance - 1], pieces)
        slot = meta[distance]
        work_gram(
            slot, slot < meta[ways], whole.at[distance - 1], left, right_stats, left_out, right_out, writes
        )
    writes.wait()


def last_kernel(ways, meta, a, b, root, right, moment, left, right_stats, precond, *rest):
    norms, rest = rest[:ways], rest[ways + 3 :]
    update, moment_out, left_out, right_out, whole, stage, sems = rest
    writes = Writes(stage, sems)
    total = norms[0][...]
    for part in norms[1:]:
        total = total + part[...]
    row = lax.broadcasted_iota(jnp.int32, total.shape, 0)

    def scaled(value, slot):
        live = slot < meta[ways]
        pick = lambda at: jnp.sum(jnp.where(row == at, total, 0.0), axis=0, keepdims=True)[:, 0:1]
        scale = jnp.where(live, jnp.sqrt(pick(2 * slot + 1) / jnp.where(live, pick(2 * slot), 1.0)), 0.0)
        return jnp.where(live, value * scale, 0.0)

    for distance in range(ways - 1):
        slot = meta[distance]
        writes.put(scaled(precond[slot], slot), update, slot)
    assemble(whole, (a, b))
    slot = meta[ways - 1]
    live = slot < meta[ways]
    value, _, _ = work_direct(slot, live, whole, root, right, moment, None, moment_out, writes)
    writes.put(scaled(value, slot), update, slot)
    work_gram(slot, live, whole, left, right_stats, left_out, right_out, writes)
    writes.wait()


def work(kernel, ways, meta, ins, kept, outs, staged, wholes):
    width = ins[0].shape[-1]
    rows = outs[0].shape[1]
    args = [meta] + [in_vmem(x) for x in ins]
    specs = [IN_SMEM] + [IN_VMEM] * len(ins)
    alias = {}
    for array, near, out in kept:
        if out is not None:
            alias[len(args)] = out
        args.append(in_vmem(array) if near else in_hbm(array))
        specs.append(IN_VMEM if near else IN_HBM)
    spec_of = lambda ref: IN_HBM if ref.memory_space == pltpu.HBM else IN_VMEM
    return call(
        functools.partial(kernel, ways),
        tuple(outs),
        args,
        specs,
        tuple(spec_of(x) for x in outs),
        [
            VMEM((width, width) if wholes == 1 else (wholes, width, width), jnp.bfloat16),
            VMEM((staged, rows, width), jnp.float32),
            pltpu.SemaphoreType.DMA((staged,)),
        ],
        input_output_aliases=alias,
    )


def on_device_direct(
    grads, left_stats, right_stats, left_root, right_root, second_moment, slot_block, counts
):
    ways, chunks = lax.axis_size("dp"), 2
    owners, slots = slot_block.shape
    first = (left_root[0], right_root[0], second_moment[0])
    second = (left_stats[0], right_stats[0])
    parts = []
    for part in range(chunks):
        dealt = deal(slot_block, counts, grads[0], ways, part, chunks)
        parts.append(list(dealt[:1]))
        for k in range(1, ways):
            parts[part].append(exchange(dealt[k], "dp", k))
    meta, lent = ready(counts, left_root[0], second_moment[0], ways)
    lent = exchange(lent, "dp", ways - 1)
    first = fetch(first)
    second = fetch(second)
    blocks = []
    for part in range(chunks):
        same, other = sort(counts, parts[part], owners)
        other = exchange(other, "fsdp", 1)
        sent = pair(same, other)
        got = [None] * len(sent)
        for k in range(len(sent)):
            got[k] = exchange(sent[k], "fsdp", 2 * k + 2)
        blocks.append(land(same, other, got))
    side, over = [], []
    for part in range(chunks):
        side.append(exchange(blocks[part], "dp", 1))
        over.append(exchange(blocks[part], "dp", 2))
    relay0 = exchange(side[0], "dp", 2)
    relay1 = exchange(over[1], "dp", 1)

    state = (slots,) + left_stats.shape[2:]
    near, far = pltpu.VMEM(state, jnp.float32), pltpu.HBM(state, jnp.float32)
    norm = pltpu.VMEM((-(-2 * slots // 8) * 8, 128), jnp.float32)
    ins = (*blocks, *first, *second, lent)
    precond, moment, norms, left, right = work(own_kernel, ways, meta, ins, (), (near, far, norm, far, far), 3, 1)
    kept = ((precond, True, 0), (moment, False, 1), (norms, True, None))
    precond, moment, norms = work(beside_kernel, ways, meta, (*side, *over, *first), kept, (near, far, norm), 2, 2)
    all_norms = [norms]
    for k in range(1, ways):
        all_norms.append(exchange(norms, "dp", k))
    kept = ((left, False, 0), (right, False, 1))
    left, right = work(gram_kernel, ways, meta, (*side, *over, *second), kept, (far, far), 4, 2)
    ins = (relay0, relay1, *first, *second, precond, *all_norms)
    kept = ((moment, False, 1), (left, False, 2), (right, False, 3))
    update, second_new, left_new, right_new = work(last_kernel, ways, meta, ins, kept, (far,) * 4, ways + 3, 1)
    return (left_new[None], right_new[None], second_new[None], update[None])


def on_device(
    grads, left_stats, right_stats, left_root, right_root, second_moment, slot_block, counts
):
    slot_count = slot_block.shape[1]
    owner_count = slot_block.shape[0]
    block_order = left_root.shape[3]
    partial_value = grads[0]
    block_count = partial_value.shape[0]
    slab_rows = partial_value.shape[1]
    flat_slots = slot_block.reshape(-1)
    live_slots = (jnp.arange(slot_count, dtype=jnp.int32)[None, :] < counts[:, None]).reshape(-1)
    flat_partial = partial_value.reshape(block_count, slab_rows * block_order).astype(jnp.float32)
    summed = lax.psum_scatter(
        flat_partial.astype(jnp.bfloat16), "dp", scatter_dimension=1, tiled=True
    )
    picked = jnp.where(live_slots[:, None], summed[flat_slots], jnp.zeros((), jnp.bfloat16))
    received = lax.all_to_all(picked, "fsdp", split_axis=0, concat_axis=1, tiled=True)
    piece_width = summed.shape[1]
    received = received.reshape(slot_count, owner_count, piece_width)
    gathered = lax.all_gather(received, "dp", axis=2, tiled=True)
    grad_full = gathered.reshape(slot_count, block_order, block_order)
    slab_width = block_order // lax.axis_size("dp")
    row_start = lax.axis_index("dp") * slab_width
    row_grad = lax.dynamic_slice_in_dim(grad_full, row_start, slab_width, 1)
    column_grad = lax.dynamic_slice_in_dim(grad_full, row_start, slab_width, 2)
    owned_here = jnp.arange(slot_count, dtype=jnp.int32) < counts[lax.axis_index("fsdp")]
    keep_mask = owned_here[:, None, None]
    left_term = jnp.einsum("crk,cjk->crj", row_grad, grad_full, preferred_element_type=jnp.float32)
    right_term = jnp.einsum(
        "ckr,ckj->crj", column_grad, grad_full, preferred_element_type=jnp.float32
    )
    left_old = left_stats[0]
    right_old = right_stats[0]
    left_new = jnp.where(
        keep_mask, SHAMPOO_BETA * left_old + (1.0 - SHAMPOO_BETA) * left_term, left_old
    )
    right_new = jnp.where(
        keep_mask, SHAMPOO_BETA * right_old + (1.0 - SHAMPOO_BETA) * right_term, right_old
    )
    left_half = jnp.einsum(
        "crk,ckj->crj", left_root[0], grad_full, preferred_element_type=jnp.float32
    ).astype(jnp.bfloat16)
    precond = jnp.einsum(
        "crk,ckj->crj", left_half, right_root[0], preferred_element_type=jnp.float32
    )
    row_values = row_grad.astype(jnp.float32)
    moment_old = second_moment[0]
    second_new = jnp.where(
        keep_mask, ADAM_BETA * moment_old + (1.0 - ADAM_BETA) * row_values * row_values, moment_old
    )
    adam = row_values / (jnp.sqrt(second_new) + EPSILON)
    precond_sum, adam_sum = lax.psum(
        (jnp.sum(precond * precond, axis=(1, 2)), jnp.sum(adam * adam, axis=(1, 2))), "dp"
    )
    graft_scale = jnp.where(
        owned_here, jnp.sqrt(adam_sum / jnp.where(owned_here, precond_sum, 1.0)), 0.0
    )
    update = precond * graft_scale[:, None, None]
    return (left_new[None], right_new[None], second_new[None], update[None])


def solution(mesh):
    in_specs = (
        P("dp", None, "fsdp", None),
        P("fsdp", None, "dp", None),
        P("fsdp", None, "dp", None),
        P("fsdp", None, "dp", None),
        P("fsdp", None, None, None),
        P("fsdp", None, "dp", None),
        P(),
        P(),
    )
    out_specs = (
        P("fsdp", None, "dp", None),
        P("fsdp", None, "dp", None),
        P("fsdp", None, "dp", None),
        P("fsdp", None, "dp", None),
    )

    ways, owners = mesh.shape["dp"], mesh.shape["fsdp"]
    square = ways == 4 and owners % 2 == 0 and owners & (owners - 1) == 0

    def fits(args):
        return square and args[6].shape[1] == ways and args[0].shape[1] % ways == 0

    def body(*args):
        return (on_device_direct if fits(args) else on_device)(*args)

    return jax.shard_map(body, mesh=mesh, in_specs=in_specs, out_specs=out_specs, check_vma=False)
```

```python
import functools

import jax
import jax.numpy as jnp
from jax import lax
from jax.experimental import pallas as pl
from jax.experimental.pallas import tpu as pltpu
from jax.sharding import PartitionSpec as P


SHAMPOO_BETA = 0.998
ADAM_BETA = 0.95
EPSILON = 1e-08
SMALL = 8 * 1024 * 1024
SMEM = pltpu.SMEM
VMEM = pltpu.VMEM


def exchange(value, axis, distance):
    size = lax.axis_size(axis)
    return lax.ppermute(value, axis, [(i, i ^ distance) for i in range(size)])


def in_hbm(value):
    return pltpu.with_memory_space_constraint(value, pltpu.HBM)


def in_vmem(value):
    return pltpu.with_memory_space_constraint(value, pltpu.VMEM)


def in_smem(value):
    return pltpu.with_memory_space_constraint(value, pltpu.SMEM)


def call(kernel, out, ins, in_specs, out_specs, scratch=(), **more):
    return pl.pallas_call(
        kernel,
        out_shape=out,
        in_specs=in_specs,
        out_specs=out_specs,
        scratch_shapes=list(scratch),
        compiler_params=pltpu.CompilerParams(vmem_limit_bytes=SMALL),
        cost_estimate=pl.CostEstimate(flops=10_000_000, bytes_accessed=1_000_000, transcendentals=0),
        **more,
    )(*ins)


IN_SMEM = pl.BlockSpec(memory_space=SMEM)
IN_VMEM = pl.BlockSpec(memory_space=VMEM)
IN_HBM = pl.BlockSpec(memory_space=pltpu.HBM)


def first_place(counts, owner):
    start = jnp.int32(0)
    for at in range(counts.shape[0]):
        start = start + jnp.where(at < owner, counts[at], 0)
    return start


def send_blocks(part, chunks, order, grads, outs, sems):
    ways, group, rows = len(outs), outs[0].shape[0], grads.shape[1] // chunks
    me = lax.axis_index("dp")
    copies = []
    for distance in list(range(1, ways)) + [0]:
        for at in range(group):
            block = order[at * ways + (me ^ distance)]
            sem = sems.at[distance * group + at]
            copy = pltpu.make_async_copy(grads.at[block, pl.ds(part * rows, rows)], outs[distance].at[at], sem)
            copy.start()
            copies.append(copy)
    return copies


def deal_kernel(chunks, slot_block, counts, grads, *rest):
    outs, (order, meta, picks, sems) = rest[:-4], rest[-4:]
    ways = len(outs)
    cap, owners = slot_block.shape
    place = jnp.int32(0)
    for owner in range(owners):
        for slot in range(cap):

            @pl.when(slot < counts[owner])
            def _():
                order[place + slot] = slot_block[slot, owner]

        place = place + counts[owner]
    copies = send_blocks(0, chunks, order, grads, outs, sems)
    me, owner_here = lax.axis_index("dp"), lax.axis_index("fsdp")
    start = first_place(counts, owner_here)
    for distance in range(ways):
        meta[distance] = ((me ^ distance) - start + owners * ways * 2) % ways
    meta[ways] = counts[owner_here]
    for distance in range(owners):
        owner = owner_here ^ distance
        start = first_place(counts, owner)
        slot = (me - start + owners * ways * 2) % ways
        picks[distance] = jnp.where(slot < counts[owner], (start + slot) // ways, 0)
    for copy in copies:
        copy.wait()


def deal(slot_block, counts, grads, ways, chunks):
    blocks, rows, width = grads.shape
    sizes = (blocks, ways + 1, counts.shape[0])
    *outs, order, meta, picks = call(
        functools.partial(deal_kernel, chunks),
        (pltpu.VMEM((blocks // ways, rows // chunks, width), grads.dtype),) * ways
        + tuple(pltpu.SMEM((size,), jnp.int32) for size in sizes),
        (in_hbm(slot_block.T), in_hbm(counts), in_hbm(grads)),
        [IN_SMEM, IN_SMEM, IN_HBM],
        (IN_VMEM,) * ways + (IN_SMEM,) * 3,
        [pltpu.SemaphoreType.DMA((blocks,))],
    )
    return outs, order, meta, picks


def more_kernel(part, chunks, order, meta, grads, root, moment, *rest):
    outs, (lent, wide, sems, more) = rest[:-4], rest[-4:]
    copies = send_blocks(part, chunks, order, grads, outs, sems)
    slot = meta[len(outs) - 1]
    far = pltpu.make_async_copy(moment.at[slot], wide, more.at[0])
    near = pltpu.make_async_copy(root.at[slot], lent.at[0], more.at[1])
    far.start()
    near.start()
    far.wait()
    lent[1] = wide[...].astype(lent.dtype)
    for copy in (near, *copies):
        copy.wait()


def deal_more(order, meta, grads, root, moment, ways, part, chunks):
    blocks, rows, width = grads.shape
    _, high, wide = root.shape
    return call(
        functools.partial(more_kernel, part, chunks),
        (pltpu.VMEM((blocks // ways, rows // chunks, width), grads.dtype),) * ways
        + (pltpu.VMEM((2, high, wide), jnp.bfloat16),),
        (in_smem(order), in_smem(meta), in_hbm(grads), in_hbm(root), in_hbm(moment)),
        [IN_SMEM, IN_SMEM] + [IN_HBM] * 3,
        (IN_VMEM,) * (ways + 1),
        [VMEM((high, wide), jnp.float32), pltpu.SemaphoreType.DMA((blocks,)), pltpu.SemaphoreType.DMA((2,))],
    )


def fetch_kernel(*refs):
    count = len(refs) // 2
    sources, outs, sems = refs[:count], refs[count:-1], refs[-1]
    copies = [pltpu.make_async_copy(a, b, sems.at[at]) for at, (a, b) in enumerate(zip(sources, outs))]
    for copy in copies:
        copy.start()
    for copy in copies:
        copy.wait()


def fetch(arrays):
    return call(
        fetch_kernel,
        tuple(pltpu.VMEM(x.shape, x.dtype) for x in arrays),
        [in_hbm(x) for x in arrays],
        [IN_HBM] * len(arrays),
        (IN_VMEM,) * len(arrays),
        [pltpu.SemaphoreType.DMA((len(arrays),))],
    )


def add_parts(parts, held):
    total = parts[0][...].astype(jnp.float32)
    for part in parts[1:]:
        total = total + part[...].astype(jnp.float32)
    held[...] = total.astype(held.dtype)


def sort_kernel(picks, *rest):
    parts, (same, other, held) = rest[:-3], rest[-3:]
    add_parts(parts, held)
    for distance in range(same.shape[0]):
        same[distance] = held[picks[2 * distance]]
        other[distance] = held[picks[2 * distance + 1]]


def sort(picks, parts, owners):
    group = parts[0].shape
    half = pltpu.VMEM((owners // 2,) + group[1:], parts[0].dtype)
    return call(
        sort_kernel,
        (half, half),
        (in_smem(picks), *[in_vmem(x) for x in parts]),
        [IN_SMEM] + [IN_VMEM] * len(parts),
        (IN_VMEM, IN_VMEM),
        [VMEM(group, parts[0].dtype)],
    )


def pair_kernel(same, other, *outs):
    for at, out in enumerate(outs):
        out[0] = same[at + 1]
        out[1] = other[at + 1]


def pair(same, other):
    out = pltpu.VMEM((2,) + same.shape[1:], same.dtype)
    count = same.shape[0] - 1
    return call(pair_kernel, (out,) * count, (in_vmem(same), in_vmem(other)), [IN_VMEM] * 2, (IN_VMEM,) * count)


def land_kernel(same, other, *rest):
    got, out = rest[:-1], rest[-1]
    me = lax.axis_index("fsdp")
    out[me] = same[0]
    out[me ^ 1] = other[0]
    for at, pieces in enumerate(got):
        out[me ^ (2 * at + 2)] = pieces[0]
        out[me ^ (2 * at + 3)] = pieces[1]


def land(same, other, got):
    out = pltpu.VMEM((2 * same.shape[0],) + same.shape[1:], same.dtype)
    ins = [in_vmem(x) for x in (same, other, *got)]
    return call(land_kernel, out, ins, [IN_VMEM] * len(ins), IN_VMEM)


def assemble(whole, pieces):
    slabs, rows, _ = pieces[0].shape
    for slab in range(slabs):
        for part, piece in enumerate(pieces):
            at = (slab * len(pieces) + part) * rows
            whole[at : at + rows, :] = piece[slab]


def precondition(root, whole, right):
    half = jnp.dot(root, whole[...], preferred_element_type=jnp.float32).astype(jnp.bfloat16)
    return jnp.dot(half, right, preferred_element_type=jnp.float32)


def own_rows(device, rows):
    return pl.ds(pl.multiple_of(device * rows, rows), rows)


def second_of(live, old, values):
    return jnp.where(live, ADAM_BETA * old + (1.0 - ADAM_BETA) * values * values, old)


def norms_of(precond, values, moment):
    adam = values / (jnp.sqrt(moment) + EPSILON)
    return jnp.sum(precond * precond), jnp.sum(adam * adam)


def put_norms(kept, slot, sums):
    row = lax.broadcasted_iota(jnp.int32, kept.shape, 0)
    return jnp.where(row == 2 * slot, sums[0], jnp.where(row == 2 * slot + 1, sums[1], kept))


class Writes:
    def __init__(self, stage, sems):
        self.stage, self.sems, self.copies = stage, sems, []

    def put(self, value, out, slot):
        at = len(self.copies)
        self.stage[at] = value
        self.copies.append(pltpu.make_async_copy(self.stage.at[at], out.at[slot], self.sems.at[at]))
        self.copies[-1].start()

    def wait(self):
        for copy in self.copies:
            copy.wait()


def work_direct(slot, live, whole, root, right, moment, precond_out, moment_out, writes):
    precond = precondition(root[slot], whole, right[slot])
    if precond_out is not None:
        precond_out[slot] = precond
    values = whole[own_rows(lax.axis_index("dp"), root.shape[1]), :].astype(jnp.float32)
    new = second_of(live, moment[slot], values)
    writes.put(new, moment_out, slot)
    return precond, values, new


def work_gram(slot, live, whole, left, right, left_out, right_out, writes):
    rows = own_rows(lax.axis_index("dp"), left.shape[1])
    for part, dims, old, out in (
        (whole[rows, :], ((1,), (1,)), left, left_out),
        (whole[:, rows], ((0,), (0,)), right, right_out),
    ):
        term = lax.dot_general(part, whole[...], (dims, ((), ())), preferred_element_type=jnp.float32)
        kept = old[slot]
        writes.put(jnp.where(live, SHAMPOO_BETA * kept + (1.0 - SHAMPOO_BETA) * term, kept), out, slot)


def own_kernel(ways, meta, a, b, root, right, moment, left, right_stats, lent, *rest):
    precond_out, moment_out, norms, left_out, right_out, whole, stage, sems = rest
    writes = Writes(stage, sems)
    assemble(whole, (a, b))
    slot, held = meta[0], meta[ways]
    live = slot < held
    sums = norms_of(*work_direct(slot, live, whole, root, right, moment, precond_out, moment_out, writes))
    values = whole[own_rows(lax.axis_index("dp") ^ (ways - 1), root.shape[1]), :].astype(jnp.float32)
    there = precondition(lent[0], whole, right[slot])
    more = norms_of(there, values, second_of(live, lent[1].astype(jnp.float32), values))
    norms[...] = put_norms(jnp.zeros(norms.shape, jnp.float32), slot, (sums[0] + more[0], sums[1] + more[1]))
    work_gram(slot, live, whole, left, right_stats, left_out, right_out, writes)
    writes.wait()


def visit_kernel(distances, grams, ways, meta, *rest):
    rest = list(rest)
    take = lambda n: [rest.pop(0) for _ in range(n)]
    pieces = [take(2) for _ in distances]
    root, right, moment = take(3)
    stats = take(2) if grams else None
    take(2)
    (norms_in,) = take(1)
    take(2 if grams else 0)
    precond_out, moment_out, norms = take(3)
    stats_out = take(2) if grams else None
    whole, stage, sems = rest
    writes = Writes(stage, sems)
    total = norms_in[...]
    for at, distance in enumerate(distances):
        here = whole.at[at]
        assemble(here, pieces[at])
        slot = meta[distance]
        live = slot < meta[ways]
        got = work_direct(slot, live, here, root, right, moment, precond_out, moment_out, writes)
        total = put_norms(total, slot, norms_of(*got))
        if grams:
            work_gram(slot, live, here, *stats, *stats_out, writes)
    norms[...] = total
    writes.wait()


def gram_kernel(distances, ways, meta, *rest):
    pieces, rest = rest[: 2 * len(distances)], rest[2 * len(distances) :]
    left, right_stats, _, _, left_out, right_out, whole, stage, sems = rest
    writes = Writes(stage, sems)
    for at, distance in enumerate(distances):
        assemble(whole.at[at], pieces[2 * at : 2 * at + 2])
        slot = meta[distance]
        work_gram(slot, slot < meta[ways], whole.at[at], left, right_stats, left_out, right_out, writes)
    writes.wait()


def last_kernel(ways, meta, a, b, root, right, moment, left, right_stats, precond, *rest):
    norms, rest = rest[:ways], rest[ways + 3 :]
    update, moment_out, left_out, right_out, whole, stage, sems = rest
    writes = Writes(stage, sems)
    total = norms[0][...]
    for part in norms[1:]:
        total = total + part[...]
    row = lax.broadcasted_iota(jnp.int32, total.shape, 0)

    def scaled(value, slot):
        live = slot < meta[ways]
        pick = lambda at: jnp.sum(jnp.where(row == at, total, 0.0), axis=0, keepdims=True)[:, 0:1]
        scale = jnp.where(live, jnp.sqrt(pick(2 * slot + 1) / jnp.where(live, pick(2 * slot), 1.0)), 0.0)
        return jnp.where(live, value * scale, 0.0)

    for distance in range(ways - 1):
        slot = meta[distance]
        writes.put(scaled(precond[slot], slot), update, slot)
    assemble(whole, (a, b))
    slot = meta[ways - 1]
    live = slot < meta[ways]
    value, _, _ = work_direct(slot, live, whole, root, right, moment, None, moment_out, writes)
    writes.put(scaled(value, slot), update, slot)
    work_gram(slot, live, whole, left, right_stats, left_out, right_out, writes)
    writes.wait()


def work(kernel, ways, meta, ins, kept, outs, staged, wholes):
    width = ins[0].shape[-1]
    rows = outs[0].shape[1]
    args = [in_smem(meta)] + [in_vmem(x) for x in ins]
    specs = [IN_SMEM] + [IN_VMEM] * len(ins)
    alias = {}
    for array, near, out in kept:
        if out is not None:
            alias[len(args)] = out
        args.append(in_vmem(array) if near else in_hbm(array))
        specs.append(IN_VMEM if near else IN_HBM)
    spec_of = lambda ref: IN_HBM if ref.memory_space == pltpu.HBM else IN_VMEM
    return call(
        functools.partial(kernel, ways),
        tuple(outs),
        args,
        specs,
        tuple(spec_of(x) for x in outs),
        [
            VMEM(wholes + (width, width), jnp.bfloat16),
            VMEM((staged, rows, width), jnp.float32),
            pltpu.SemaphoreType.DMA((staged,)),
        ],
        input_output_aliases=alias,
    )


def on_device_direct(
    grads, left_stats, right_stats, left_root, right_root, second_moment, slot_block, counts
):
    ways, chunks = lax.axis_size("dp"), 2
    owners, slots = slot_block.shape
    first = (left_root[0], right_root[0], second_moment[0])
    second = (left_stats[0], right_stats[0])
    parts = []
    for part in range(chunks):
        if part == 0:
            dealt, order, meta, picks = deal(slot_block, counts, grads[0], ways, chunks)
        else:
            *dealt, lent = deal_more(
                order, meta, grads[0], left_root[0], second_moment[0], ways, part, chunks
            )
        parts.append(list(dealt[:1]))
        for k in range(1, ways):
            parts[part].append(exchange(dealt[k], "dp", k))
    lent = exchange(lent, "dp", ways - 1)
    first = fetch(first)
    second = fetch(second)
    blocks = []
    for part in range(chunks):
        same, other = sort(picks, parts[part], owners)
        other = exchange(other, "fsdp", 1)
        sent = pair(same, other)
        got = [None] * len(sent)
        for k in range(len(sent)):
            got[k] = exchange(sent[k], "fsdp", 2 * k + 2)
        blocks.append(land(same, other, got))
    side, over = [], []
    for part in range(chunks):
        side.append(exchange(blocks[part], "dp", 1))
        over.append(exchange(blocks[part], "dp", 2))
    relay0 = exchange(side[0], "dp", 2)
    relay1 = exchange(over[1], "dp", 1)

    state = (slots,) + left_stats.shape[2:]
    near, far = pltpu.VMEM(state, jnp.float32), pltpu.HBM(state, jnp.float32)
    norm = pltpu.VMEM((-(-2 * slots // 8) * 8, 128), jnp.float32)
    ins = (*blocks, *first, *second, lent)
    precond, moment, norms, left, right = work(own_kernel, ways, meta, ins, (), (near, far, norm, far, far), 4, ())
    kernel = functools.partial(visit_kernel, (1,), True)
    kept = ((precond, True, 0), (moment, False, 1), (norms, True, None), (left, False, 3), (right, False, 4))
    outs = (near, far, norm, far, far)
    ins = (*side, *first, *second)
    precond, moment, norms, left, right = work(kernel, ways, meta, ins, kept, outs, 3, (1,))
    kernel = functools.partial(visit_kernel, (2,), False)
    kept = ((precond, True, 0), (moment, False, 1), (norms, True, None))
    ins = (*over, *first)
    precond, moment, norms = work(kernel, ways, meta, ins, kept, (near, far, norm), 1, (1,))
    all_norms = [norms]
    for k in range(1, ways):
        all_norms.append(exchange(norms, "dp", k))
    kept = ((left, False, 0), (right, False, 1))
    kernel = functools.partial(gram_kernel, (2,))
    left, right = work(kernel, ways, meta, (*over, *second), kept, (far, far), 2, (1,))
    ins = (relay0, relay1, *first, *second, precond, *all_norms)
    kept = ((moment, False, 1), (left, False, 2), (right, False, 3))
    update, second_new, left_new, right_new = work(last_kernel, ways, meta, ins, kept, (far,) * 4, ways + 3, ())
    return (left_new[None], right_new[None], second_new[None], update[None])


def on_device(
    grads, left_stats, right_stats, left_root, right_root, second_moment, slot_block, counts
):
    slot_count = slot_block.shape[1]
    owner_count = slot_block.shape[0]
    block_order = left_root.shape[3]
    partial_value = grads[0]
    block_count = partial_value.shape[0]
    slab_rows = partial_value.shape[1]
    flat_slots = slot_block.reshape(-1)
    live_slots = (jnp.arange(slot_count, dtype=jnp.int32)[None, :] < counts[:, None]).reshape(-1)
    flat_partial = partial_value.reshape(block_count, slab_rows * block_order).astype(jnp.float32)
    summed = lax.psum_scatter(
        flat_partial.astype(jnp.bfloat16), "dp", scatter_dimension=1, tiled=True
    )
    picked = jnp.where(live_slots[:, None], summed[flat_slots], jnp.zeros((), jnp.bfloat16))
    received = lax.all_to_all(picked, "fsdp", split_axis=0, concat_axis=1, tiled=True)
    piece_width = summed.shape[1]
    received = received.reshape(slot_count, owner_count, piece_width)
    gathered = lax.all_gather(received, "dp", axis=2, tiled=True)
    grad_full = gathered.reshape(slot_count, block_order, block_order)
    slab_width = block_order // lax.axis_size("dp")
    row_start = lax.axis_index("dp") * slab_width
    row_grad = lax.dynamic_slice_in_dim(grad_full, row_start, slab_width, 1)
    column_grad = lax.dynamic_slice_in_dim(grad_full, row_start, slab_width, 2)
    owned_here = jnp.arange(slot_count, dtype=jnp.int32) < counts[lax.axis_index("fsdp")]
    keep_mask = owned_here[:, None, None]
    left_term = jnp.einsum("crk,cjk->crj", row_grad, grad_full, preferred_element_type=jnp.float32)
    right_term = jnp.einsum(
        "ckr,ckj->crj", column_grad, grad_full, preferred_element_type=jnp.float32
    )
    left_old = left_stats[0]
    right_old = right_stats[0]
    left_new = jnp.where(
        keep_mask, SHAMPOO_BETA * left_old + (1.0 - SHAMPOO_BETA) * left_term, left_old
    )
    right_new = jnp.where(
        keep_mask, SHAMPOO_BETA * right_old + (1.0 - SHAMPOO_BETA) * right_term, right_old
    )
    left_half = jnp.einsum(
        "crk,ckj->crj", left_root[0], grad_full, preferred_element_type=jnp.float32
    ).astype(jnp.bfloat16)
    precond = jnp.einsum(
        "crk,ckj->crj", left_half, right_root[0], preferred_element_type=jnp.float32
    )
    row_values = row_grad.astype(jnp.float32)
    moment_old = second_moment[0]
    second_new = jnp.where(
        keep_mask, ADAM_BETA * moment_old + (1.0 - ADAM_BETA) * row_values * row_values, moment_old
    )
    adam = row_values / (jnp.sqrt(second_new) + EPSILON)
    precond_sum, adam_sum = lax.psum(
        (jnp.sum(precond * precond, axis=(1, 2)), jnp.sum(adam * adam, axis=(1, 2))), "dp"
    )
    graft_scale = jnp.where(
        owned_here, jnp.sqrt(adam_sum / jnp.where(owned_here, precond_sum, 1.0)), 0.0
    )
    update = precond * graft_scale[:, None, None]
    return (left_new[None], right_new[None], second_new[None], update[None])


def solution(mesh):
    in_specs = (
        P("dp", None, "fsdp", None),
        P("fsdp", None, "dp", None),
        P("fsdp", None, "dp", None),
        P("fsdp", None, "dp", None),
        P("fsdp", None, None, None),
        P("fsdp", None, "dp", None),
        P(),
        P(),
    )
    out_specs = (
        P("fsdp", None, "dp", None),
        P("fsdp", None, "dp", None),
        P("fsdp", None, "dp", None),
        P("fsdp", None, "dp", None),
    )

    ways, owners = mesh.shape["dp"], mesh.shape["fsdp"]
    square = ways == 4 and owners % 2 == 0 and owners & (owners - 1) == 0

    def fits(args):
        return square and args[6].shape[1] == ways and args[0].shape[1] % ways == 0

    def body(*args):
        return (on_device_direct if fits(args) else on_device)(*args)

    return jax.shard_map(body, mesh=mesh, in_specs=in_specs, out_specs=out_specs, check_vma=False)
```

```python
import functools

import jax
import jax.numpy as jnp
from jax import lax
from jax.experimental import pallas as pl
from jax.experimental.pallas import tpu as pltpu
from jax.sharding import PartitionSpec as P


SHAMPOO_BETA = 0.998
ADAM_BETA = 0.95
EPSILON = 1e-08
SMALL = 8 * 1024 * 1024
SMEM = pltpu.SMEM
VMEM = pltpu.VMEM


def exchange(value, axis, distance):
    size = lax.axis_size(axis)
    return lax.ppermute(value, axis, [(i, i ^ distance) for i in range(size)])


def in_hbm(value):
    return pltpu.with_memory_space_constraint(value, pltpu.HBM)


def in_vmem(value):
    return pltpu.with_memory_space_constraint(value, pltpu.VMEM)


def in_smem(value):
    return pltpu.with_memory_space_constraint(value, pltpu.SMEM)


def call(kernel, out, ins, in_specs, out_specs, scratch=(), **more):
    return pl.pallas_call(
        kernel,
        out_shape=out,
        in_specs=in_specs,
        out_specs=out_specs,
        scratch_shapes=list(scratch),
        compiler_params=pltpu.CompilerParams(vmem_limit_bytes=SMALL),
        cost_estimate=pl.CostEstimate(flops=10_000_000, bytes_accessed=1_000_000, transcendentals=0),
        **more,
    )(*ins)


IN_SMEM = pl.BlockSpec(memory_space=SMEM)
IN_VMEM = pl.BlockSpec(memory_space=VMEM)
IN_HBM = pl.BlockSpec(memory_space=pltpu.HBM)


def first_place(counts, owner):
    start = jnp.int32(0)
    for at in range(counts.shape[0]):
        start = start + jnp.where(at < owner, counts[at], 0)
    return start


def send_blocks(part, chunks, order, grads, outs, sems):
    ways, group, rows = len(outs), outs[0].shape[0], grads.shape[1] // chunks
    me = lax.axis_index("dp")
    copies = []
    for distance in list(range(1, ways)) + [0]:
        for at in range(group):
            block = order[at * ways + (me ^ distance)]
            sem = sems.at[distance * group + at]
            copy = pltpu.make_async_copy(grads.at[block, pl.ds(part * rows, rows)], outs[distance].at[at], sem)
            copy.start()
            copies.append(copy)
    return copies


def deal_kernel(chunks, slot_block, counts, grads, *rest):
    outs, (order, meta, picks, sems) = rest[:-4], rest[-4:]
    ways = len(outs)
    cap, owners = slot_block.shape
    place = jnp.int32(0)
    for owner in range(owners):
        for slot in range(cap):

            @pl.when(slot < counts[owner])
            def _():
                order[place + slot] = slot_block[slot, owner]

        place = place + counts[owner]
    copies = send_blocks(0, chunks, order, grads, outs, sems)
    me, owner_here = lax.axis_index("dp"), lax.axis_index("fsdp")
    start = first_place(counts, owner_here)
    for distance in range(ways):
        meta[distance] = ((me ^ distance) - start + owners * ways * 2) % ways
    meta[ways] = counts[owner_here]
    for distance in range(owners):
        owner = owner_here ^ distance
        start = first_place(counts, owner)
        slot = (me - start + owners * ways * 2) % ways
        picks[distance] = jnp.where(slot < counts[owner], (start + slot) // ways, 0)
    for copy in copies:
        copy.wait()


def deal(slot_block, counts, grads, ways, chunks):
    blocks, rows, width = grads.shape
    sizes = (blocks, ways + 1, counts.shape[0])
    *outs, order, meta, picks = call(
        functools.partial(deal_kernel, chunks),
        (pltpu.VMEM((blocks // ways, rows // chunks, width), grads.dtype),) * ways
        + tuple(pltpu.SMEM((size,), jnp.int32) for size in sizes),
        (in_hbm(slot_block.T), in_hbm(counts), in_hbm(grads)),
        [IN_SMEM, IN_SMEM, IN_HBM],
        (IN_VMEM,) * ways + (IN_SMEM,) * 3,
        [pltpu.SemaphoreType.DMA((blocks,))],
    )
    return outs, order, meta, picks


def more_kernel(part, chunks, order, meta, grads, root, moment, *rest):
    outs, (lent, wide, sems, more) = rest[:-4], rest[-4:]
    copies = send_blocks(part, chunks, order, grads, outs, sems)
    slot = meta[len(outs) - 1]
    far = pltpu.make_async_copy(moment.at[slot], wide, more.at[0])
    near = pltpu.make_async_copy(root.at[slot], lent.at[0], more.at[1])
    far.start()
    near.start()
    far.wait()
    lent[1] = wide[...].astype(lent.dtype)
    for copy in (near, *copies):
        copy.wait()


def deal_more(order, meta, grads, root, moment, ways, part, chunks):
    blocks, rows, width = grads.shape
    _, high, wide = root.shape
    return call(
        functools.partial(more_kernel, part, chunks),
        (pltpu.VMEM((blocks // ways, rows // chunks, width), grads.dtype),) * ways
        + (pltpu.VMEM((2, high, wide), jnp.bfloat16),),
        (in_smem(order), in_smem(meta), in_hbm(grads), in_hbm(root), in_hbm(moment)),
        [IN_SMEM, IN_SMEM] + [IN_HBM] * 3,
        (IN_VMEM,) * (ways + 1),
        [VMEM((high, wide), jnp.float32), pltpu.SemaphoreType.DMA((blocks,)), pltpu.SemaphoreType.DMA((2,))],
    )


def fetch_kernel(whole, meta, *refs):
    count = len(refs) // 2
    sources, outs, sems = refs[:count], refs[count:-1], refs[-1]
    slots, held = sources[0].shape[0], meta[meta.shape[0] - 1]
    for wait in (False, True):
        for at, (source, out) in enumerate(zip(sources, outs)):
            for slot in range(slots):
                copy = pltpu.make_async_copy(source.at[slot], out.at[slot], sems.at[at * slots + slot])
                act = copy.wait if wait else copy.start
                if whole[at]:
                    act()
                else:
                    pl.when(slot < held)(act)
                    if wait:

                        @pl.when(slot >= held)
                        def _():
                            out[slot] = jnp.zeros(out.shape[1:], out.dtype)


def fetch(meta, arrays, whole):
    return call(
        functools.partial(fetch_kernel, whole),
        tuple(pltpu.VMEM(x.shape, x.dtype) for x in arrays),
        [in_smem(meta)] + [in_hbm(x) for x in arrays],
        [IN_SMEM] + [IN_HBM] * len(arrays),
        (IN_VMEM,) * len(arrays),
        [pltpu.SemaphoreType.DMA((len(arrays) * arrays[0].shape[0],))],
    )


def add_parts(parts, held):
    total = parts[0][...].astype(jnp.float32)
    for part in parts[1:]:
        total = total + part[...].astype(jnp.float32)
    held[...] = total.astype(held.dtype)


def sort_kernel(picks, *rest):
    parts, (same, other, held) = rest[:-3], rest[-3:]
    add_parts(parts, held)
    for distance in range(same.shape[0]):
        same[distance] = held[picks[2 * distance]]
        other[distance] = held[picks[2 * distance + 1]]


def sort(picks, parts, owners):
    group = parts[0].shape
    half = pltpu.VMEM((owners // 2,) + group[1:], parts[0].dtype)
    return call(
        sort_kernel,
        (half, half),
        (in_smem(picks), *[in_vmem(x) for x in parts]),
        [IN_SMEM] + [IN_VMEM] * len(parts),
        (IN_VMEM, IN_VMEM),
        [VMEM(group, parts[0].dtype)],
    )


def pair_kernel(same, other, *outs):
    for at, out in enumerate(outs):
        out[0] = same[at + 1]
        out[1] = other[at + 1]


def pair(same, other):
    out = pltpu.VMEM((2,) + same.shape[1:], same.dtype)
    count = same.shape[0] - 1
    return call(pair_kernel, (out,) * count, (in_vmem(same), in_vmem(other)), [IN_VMEM] * 2, (IN_VMEM,) * count)


def land_kernel(same, other, *rest):
    got, out = rest[:-1], rest[-1]
    me = lax.axis_index("fsdp")
    out[me] = same[0]
    out[me ^ 1] = other[0]
    for at, pieces in enumerate(got):
        out[me ^ (2 * at + 2)] = pieces[0]
        out[me ^ (2 * at + 3)] = pieces[1]


def land(same, other, got):
    out = pltpu.VMEM((2 * same.shape[0],) + same.shape[1:], same.dtype)
    ins = [in_vmem(x) for x in (same, other, *got)]
    return call(land_kernel, out, ins, [IN_VMEM] * len(ins), IN_VMEM)


def assemble(whole, pieces):
    slabs, rows, _ = pieces[0].shape
    for slab in range(slabs):
        for part, piece in enumerate(pieces):
            at = (slab * len(pieces) + part) * rows
            whole[at : at + rows, :] = piece[slab]


def precondition(root, whole, right):
    half = jnp.dot(root, whole[...], preferred_element_type=jnp.float32).astype(jnp.bfloat16)
    return jnp.dot(half, right, preferred_element_type=jnp.float32)


def own_rows(device, rows):
    return pl.ds(pl.multiple_of(device * rows, rows), rows)


def second_of(live, old, values):
    return jnp.where(live, ADAM_BETA * old + (1.0 - ADAM_BETA) * values * values, old)


def norms_of(precond, values, moment):
    adam = values / (jnp.sqrt(moment) + EPSILON)
    return jnp.sum(precond * precond), jnp.sum(adam * adam)


def put_norms(kept, slot, sums):
    row = lax.broadcasted_iota(jnp.int32, kept.shape, 0)
    return jnp.where(row == 2 * slot, sums[0], jnp.where(row == 2 * slot + 1, sums[1], kept))


class Writes:
    def __init__(self, stage, sems):
        self.stage, self.sems, self.copies = stage, sems, []

    def put(self, value, out, slot):
        at = len(self.copies)
        self.stage[at] = value
        self.copies.append(pltpu.make_async_copy(self.stage.at[at], out.at[slot], self.sems.at[at]))
        self.copies[-1].start()

    def wait(self):
        for copy in self.copies:
            copy.wait()


def work_direct(slot, live, whole, root, right, moment, precond_out, moment_out, writes):
    precond = precondition(root[slot], whole, right[slot])
    if precond_out is not None:
        precond_out[slot] = precond
    values = whole[own_rows(lax.axis_index("dp"), root.shape[1]), :].astype(jnp.float32)
    new = second_of(live, moment[slot], values)
    writes.put(new, moment_out, slot)
    return precond, values, new


def work_gram(slot, live, whole, left, right, left_out, right_out, writes):
    rows = own_rows(lax.axis_index("dp"), left.shape[1])
    for part, dims, old, out in (
        (whole[rows, :], ((1,), (1,)), left, left_out),
        (whole[:, rows], ((0,), (0,)), right, right_out),
    ):
        term = lax.dot_general(part, whole[...], (dims, ((), ())), preferred_element_type=jnp.float32)
        kept = old[slot]
        writes.put(jnp.where(live, SHAMPOO_BETA * kept + (1.0 - SHAMPOO_BETA) * term, kept), out, slot)


def own_kernel(ways, meta, a, b, root, right, moment, left, right_stats, lent, *rest):
    precond_out, moment_out, norms, left_out, right_out, whole, stage, sems = rest
    writes = Writes(stage, sems)
    assemble(whole, (a, b))
    slot, held = meta[0], meta[ways]
    live = slot < held
    sums = norms_of(*work_direct(slot, live, whole, root, right, moment, precond_out, moment_out, writes))
    values = whole[own_rows(lax.axis_index("dp") ^ (ways - 1), root.shape[1]), :].astype(jnp.float32)
    there = precondition(lent[0], whole, right[slot])
    more = norms_of(there, values, second_of(live, lent[1].astype(jnp.float32), values))
    norms[...] = put_norms(jnp.zeros(norms.shape, jnp.float32), slot, (sums[0] + more[0], sums[1] + more[1]))
    work_gram(slot, live, whole, left, right_stats, left_out, right_out, writes)
    writes.wait()


def visit_kernel(distances, grams, ways, meta, *rest):
    rest = list(rest)
    take = lambda n: [rest.pop(0) for _ in range(n)]
    pieces = [take(2) for _ in distances]
    root, right, moment = take(3)
    stats = take(2) if grams else None
    take(2)
    (norms_in,) = take(1)
    take(2 if grams else 0)
    precond_out, moment_out, norms = take(3)
    stats_out = take(2) if grams else None
    whole, stage, sems = rest
    writes = Writes(stage, sems)
    total = norms_in[...]
    for at, distance in enumerate(distances):
        here = whole.at[at]
        assemble(here, pieces[at])
        slot = meta[distance]
        live = slot < meta[ways]
        got = work_direct(slot, live, here, root, right, moment, precond_out, moment_out, writes)
        total = put_norms(total, slot, norms_of(*got))
        if grams:
            work_gram(slot, live, here, *stats, *stats_out, writes)
    norms[...] = total
    writes.wait()


def gram_kernel(distances, ways, meta, *rest):
    pieces, rest = rest[: 2 * len(distances)], rest[2 * len(distances) :]
    left, right_stats, _, _, left_out, right_out, whole, stage, sems = rest
    writes = Writes(stage, sems)
    for at, distance in enumerate(distances):
        assemble(whole.at[at], pieces[2 * at : 2 * at + 2])
        slot = meta[distance]
        work_gram(slot, slot < meta[ways], whole.at[at], left, right_stats, left_out, right_out, writes)
    writes.wait()


def last_kernel(ways, meta, a, b, root, right, moment, left, right_stats, precond, *rest):
    norms, rest = rest[:ways], rest[ways + 3 :]
    update, moment_out, left_out, right_out, whole, stage, sems = rest
    writes = Writes(stage, sems)
    total = norms[0][...]
    for part in norms[1:]:
        total = total + part[...]
    row = lax.broadcasted_iota(jnp.int32, total.shape, 0)

    def scaled(value, slot):
        live = slot < meta[ways]
        pick = lambda at: jnp.sum(jnp.where(row == at, total, 0.0), axis=0, keepdims=True)[:, 0:1]
        scale = jnp.where(live, jnp.sqrt(pick(2 * slot + 1) / jnp.where(live, pick(2 * slot), 1.0)), 0.0)
        return jnp.where(live, value * scale, 0.0)

    for distance in range(ways - 1):
        slot = meta[distance]
        writes.put(scaled(precond[slot], slot), update, slot)
    assemble(whole, (a, b))
    slot = meta[ways - 1]
    live = slot < meta[ways]
    value, _, _ = work_direct(slot, live, whole, root, right, moment, None, moment_out, writes)
    writes.put(scaled(value, slot), update, slot)
    work_gram(slot, live, whole, left, right_stats, left_out, right_out, writes)
    writes.wait()


def work(kernel, ways, meta, ins, kept, outs, staged, wholes):
    width = ins[0].shape[-1]
    rows = outs[0].shape[1]
    args = [in_smem(meta)] + [in_vmem(x) for x in ins]
    specs = [IN_SMEM] + [IN_VMEM] * len(ins)
    alias = {}
    for array, near, out in kept:
        if out is not None:
            alias[len(args)] = out
        args.append(in_vmem(array) if near else in_hbm(array))
        specs.append(IN_VMEM if near else IN_HBM)
    spec_of = lambda ref: IN_HBM if ref.memory_space == pltpu.HBM else IN_VMEM
    return call(
        functools.partial(kernel, ways),
        tuple(outs),
        args,
        specs,
        tuple(spec_of(x) for x in outs),
        [
            VMEM(wholes + (width, width), jnp.bfloat16),
            VMEM((staged, rows, width), jnp.float32),
            pltpu.SemaphoreType.DMA((staged,)),
        ],
        input_output_aliases=alias,
    )


def on_device_direct(
    grads, left_stats, right_stats, left_root, right_root, second_moment, slot_block, counts
):
    ways, chunks = lax.axis_size("dp"), 2
    owners, slots = slot_block.shape
    first = (left_root[0], right_root[0], second_moment[0])
    second = (left_stats[0], right_stats[0])
    parts = []
    for part in range(chunks):
        if part == 0:
            dealt, order, meta, picks = deal(slot_block, counts, grads[0], ways, chunks)
        else:
            *dealt, lent = deal_more(
                order, meta, grads[0], left_root[0], second_moment[0], ways, part, chunks
            )
        parts.append(list(dealt[:1]))
        for k in range(1, ways):
            parts[part].append(exchange(dealt[k], "dp", k))
    lent = exchange(lent, "dp", ways - 1)
    first = fetch(meta, first, (False, False, True))
    second = fetch(meta, second, (True, True))
    blocks = []
    for part in range(chunks):
        same, other = sort(picks, parts[part], owners)
        other = exchange(other, "fsdp", 1)
        sent = pair(same, other)
        got = [None] * len(sent)
        for k in range(len(sent)):
            got[k] = exchange(sent[k], "fsdp", 2 * k + 2)
        blocks.append(land(same, other, got))
    side, over = [], []
    for part in range(chunks):
        side.append(exchange(blocks[part], "dp", 1))
        over.append(exchange(blocks[part], "dp", 2))
    relay0 = exchange(side[0], "dp", 2)
    relay1 = exchange(over[1], "dp", 1)

    state = (slots,) + left_stats.shape[2:]
    near, far = pltpu.VMEM(state, jnp.float32), pltpu.HBM(state, jnp.float32)
    norm = pltpu.VMEM((-(-2 * slots // 8) * 8, 128), jnp.float32)
    ins = (*blocks, *first, *second, lent)
    precond, moment, norms, left, right = work(own_kernel, ways, meta, ins, (), (near, far, norm, far, far), 4, ())
    kernel = functools.partial(visit_kernel, (1,), True)
    kept = ((precond, True, 0), (moment, False, 1), (norms, True, None), (left, False, 3), (right, False, 4))
    outs = (near, far, norm, far, far)
    ins = (*side, *first, *second)
    precond, moment, norms, left, right = work(kernel, ways, meta, ins, kept, outs, 3, (1,))
    kernel = functools.partial(visit_kernel, (2,), False)
    kept = ((precond, True, 0), (moment, False, 1), (norms, True, None))
    ins = (*over, *first)
    precond, moment, norms = work(kernel, ways, meta, ins, kept, (near, far, norm), 1, (1,))
    all_norms = [norms]
    for k in range(1, ways):
        all_norms.append(exchange(norms, "dp", k))
    kept = ((left, False, 0), (right, False, 1))
    kernel = functools.partial(gram_kernel, (2,))
    left, right = work(kernel, ways, meta, (*over, *second), kept, (far, far), 2, (1,))
    ins = (relay0, relay1, *first, *second, precond, *all_norms)
    kept = ((moment, False, 1), (left, False, 2), (right, False, 3))
    update, second_new, left_new, right_new = work(last_kernel, ways, meta, ins, kept, (far,) * 4, ways + 3, ())
    return (left_new[None], right_new[None], second_new[None], update[None])


def on_device(
    grads, left_stats, right_stats, left_root, right_root, second_moment, slot_block, counts
):
    slot_count = slot_block.shape[1]
    owner_count = slot_block.shape[0]
    block_order = left_root.shape[3]
    partial_value = grads[0]
    block_count = partial_value.shape[0]
    slab_rows = partial_value.shape[1]
    flat_slots = slot_block.reshape(-1)
    live_slots = (jnp.arange(slot_count, dtype=jnp.int32)[None, :] < counts[:, None]).reshape(-1)
    flat_partial = partial_value.reshape(block_count, slab_rows * block_order).astype(jnp.float32)
    summed = lax.psum_scatter(
        flat_partial.astype(jnp.bfloat16), "dp", scatter_dimension=1, tiled=True
    )
    picked = jnp.where(live_slots[:, None], summed[flat_slots], jnp.zeros((), jnp.bfloat16))
    received = lax.all_to_all(picked, "fsdp", split_axis=0, concat_axis=1, tiled=True)
    piece_width = summed.shape[1]
    received = received.reshape(slot_count, owner_count, piece_width)
    gathered = lax.all_gather(received, "dp", axis=2, tiled=True)
    grad_full = gathered.reshape(slot_count, block_order, block_order)
    slab_width = block_order // lax.axis_size("dp")
    row_start = lax.axis_index("dp") * slab_width
    row_grad = lax.dynamic_slice_in_dim(grad_full, row_start, slab_width, 1)
    column_grad = lax.dynamic_slice_in_dim(grad_full, row_start, slab_width, 2)
    owned_here = jnp.arange(slot_count, dtype=jnp.int32) < counts[lax.axis_index("fsdp")]
    keep_mask = owned_here[:, None, None]
    left_term = jnp.einsum("crk,cjk->crj", row_grad, grad_full, preferred_element_type=jnp.float32)
    right_term = jnp.einsum(
        "ckr,ckj->crj", column_grad, grad_full, preferred_element_type=jnp.float32
    )
    left_old = left_stats[0]
    right_old = right_stats[0]
    left_new = jnp.where(
        keep_mask, SHAMPOO_BETA * left_old + (1.0 - SHAMPOO_BETA) * left_term, left_old
    )
    right_new = jnp.where(
        keep_mask, SHAMPOO_BETA * right_old + (1.0 - SHAMPOO_BETA) * right_term, right_old
    )
    left_half = jnp.einsum(
        "crk,ckj->crj", left_root[0], grad_full, preferred_element_type=jnp.float32
    ).astype(jnp.bfloat16)
    precond = jnp.einsum(
        "crk,ckj->crj", left_half, right_root[0], preferred_element_type=jnp.float32
    )
    row_values = row_grad.astype(jnp.float32)
    moment_old = second_moment[0]
    second_new = jnp.where(
        keep_mask, ADAM_BETA * moment_old + (1.0 - ADAM_BETA) * row_values * row_values, moment_old
    )
    adam = row_values / (jnp.sqrt(second_new) + EPSILON)
    precond_sum, adam_sum = lax.psum(
        (jnp.sum(precond * precond, axis=(1, 2)), jnp.sum(adam * adam, axis=(1, 2))), "dp"
    )
    graft_scale = jnp.where(
        owned_here, jnp.sqrt(adam_sum / jnp.where(owned_here, precond_sum, 1.0)), 0.0
    )
    update = precond * graft_scale[:, None, None]
    return (left_new[None], right_new[None], second_new[None], update[None])


def solution(mesh):
    in_specs = (
        P("dp", None, "fsdp", None),
        P("fsdp", None, "dp", None),
        P("fsdp", None, "dp", None),
        P("fsdp", None, "dp", None),
        P("fsdp", None, None, None),
        P("fsdp", None, "dp", None),
        P(),
        P(),
    )
    out_specs = (
        P("fsdp", None, "dp", None),
        P("fsdp", None, "dp", None),
        P("fsdp", None, "dp", None),
        P("fsdp", None, "dp", None),
    )

    ways, owners = mesh.shape["dp"], mesh.shape["fsdp"]
    square = ways == 4 and owners % 2 == 0 and owners & (owners - 1) == 0

    def fits(args):
        return square and args[6].shape[1] == ways and args[0].shape[1] % ways == 0

    def body(*args):
        return (on_device_direct if fits(args) else on_device)(*args)

    return jax.shard_map(body, mesh=mesh, in_specs=in_specs, out_specs=out_specs, check_vma=False)
```
